128 devices in a mesh: rep: 2 (over core), dp: 64 (over x, y, z).
Axes of the slice: x: 4, y: 4, z: 4, core: 2. Of those that a mesh axis runs over, the one named last changes fastest.
Arguments:
- a: bfloat16 [128, 2, 4096, 1024], P(('rep', 'dp')), parts along dimension 0
- g: bfloat16 [128, 2, 4096, 3200], P(('rep', 'dp')), parts along dimension 0
Outputs:
- output: bfloat16 [4, 1024, 3200], P('rep'), parts along dimension 0
There are 2 independent parts. The reference program is written for one: setup_inputs(seed, part) draws one part's arguments, and reference() takes and returns one part's arrays. A program takes and returns all parts, laid end to end along the dimension named above; each array names one.
All inputs are finite; a program needn't handle non-finite values.
Results may differ from the reference program's by a relative error of at most 0.012.
Values are sent between devices in bfloat16 or wider.
A program may use at most 1.5 GiB of HBM per device.

```python
import jax
import jax.numpy as jnp
from jax import lax

DEVICES = 64
MATRICES = 2
TOKENS = 4096
D = 1024
FF = 3200


def setup_inputs(seed: int = 0, part: int = 0) -> dict:
    ka, kg, ks = (jax.random.fold_in(k, part) for k in jax.random.split(jax.random.key(seed), 3))
    size = 2.0 ** jax.random.uniform(ks, (DEVICES, MATRICES, 1, 1), jnp.float32, -1.0, 1.0)
    a = jax.random.normal(ka, (DEVICES, MATRICES, TOKENS, D), jnp.float32)
    g = size * jax.random.normal(kg, (DEVICES, MATRICES, TOKENS, FF), jnp.float32) * (DEVICES * TOKENS) ** -0.5
    return {"a": a.astype(jnp.bfloat16), "g": g.astype(jnp.bfloat16)}


def reference(a, g):
    def take(so_far, one):
        term = jnp.einsum("ntd,ntf->ndf", *one, preferred_element_type=jnp.float32).astype(jnp.bfloat16)
        return so_far + term.astype(jnp.float32), None

    return lax.scan(take, jnp.zeros((MATRICES, D, FF), jnp.float32), (a, g))[0].astype(jnp.bfloat16)
```

```python
import functools

import jax
import jax.numpy as jnp
from jax import lax
from jax.experimental import pallas as pl
from jax.experimental.pallas import tpu as pltpu
from jax.sharding import PartitionSpec as P

MESH = pl.DeviceIdType.MESH
BF, F32 = jnp.bfloat16, jnp.float32

D, FF, TOKENS = 1024, 3200, 4096
COLS = 256
PER = FF // COLS
ITEMS = 2 * PER + 1
MIXED = PER
KB = 1024
LAGS = (0, 2, 4, 5, 7, 8, 9, 10, 12, 14, 16)
SLOTS = LAGS[10] + 1
FSLOTS = 8


def kernel(a_hbm, g_hbm, out, a_buf, g_buf, acc, terms, r1, c1, f1, s2, r2, f2, s3, r3,
           a_sem, g_sem, send, opp1, rest1, opp2, rest2, in3, ag3, fwd2, ag2, fwd1, ag1):
    dp = lax.axis_index("dp")
    x, y, z = dp // 16, (dp // 4) % 4, dp % 4

    def axis(k):
        w0, w1, w2 = (1 - k) * (2 - k) // 2, k * (2 - k), k * (k - 1) // 2
        c, s = x * w0 + y * w1 + z * w2, 16 * w0 + 4 * w1 + w2
        return c, lambda d: dp + s * ((c + d) % 4 - c)

    def rows(start, size):
        return pl.ds(pl.multiple_of(start, 16), size)

    def a_copy(n, j):
        return pltpu.make_async_copy(a_hbm.at[0, n, pl.ds(j * KB, KB), :], a_buf.at[pl.ds(j * KB, KB), :], a_sem.at[j])

    def g_copy(n, first, width, slot, at):
        return pltpu.make_async_copy(
            g_hbm.at[0, n, :, pl.ds(first, width)], g_buf.at[slot, :, pl.ds(at, width)], g_sem.at[slot])

    def g_start(t):
        @pl.when((t < MIXED) | ((t > MIXED) & (t < ITEMS)))
        def _():
            n = t // (MIXED + 1)
            b = t - n * (MIXED + 1)
            g_copy(n, pl.multiple_of(b * COLS, COLS), COLS, t % 2, 0).start()

        @pl.when(t == MIXED)
        def _():
            g_copy(0, PER * COLS, 128, MIXED % 2, 0).start()
            g_copy(1, PER * COLS, 128, MIXED % 2, 128).start()

    def g_wait(t):
        g_copy(0, 0, COLS, t % 2, 0).wait()

    def dot(a, g):
        return lax.dot_general(a, g, (((0,), (0,)), ((), ())), preferred_element_type=F32)

    def blocked(slot, cols, row0, before, after):
        for j in range(TOKENS // KB):
            before(j)
            part = dot(a_buf[pl.ds(j * KB, KB), :], g_buf[slot, pl.ds(j * KB, KB), cols])
            if j == 0:
                acc[:, cols] = part
            else:
                acc[:, cols] += part
            after(j)
        terms[pl.ds(row0, D), cols] = acc[:, cols].astype(BF)

    def push(i, src, dst, sem, to):
        pltpu.make_async_remote_copy(
            src_ref=src, dst_ref=dst, send_sem=send.at[i % SLOTS], recv_sem=sem,
            device_id={"dp": to}, device_id_type=MESH).start()

    def arrived(ref, sem):
        pltpu.make_async_copy(ref, ref, sem).wait()

    def place(i):
        k = i % 3
        return axis(k), axis((k + 1) % 3), axis((k + 2) % 3)

    def up(ref):
        return ref[...].astype(F32)

    def e0(i):
        (c, to), _, _ = place(i)
        base = i * D
        q = lambda d, h: rows(base + 256 * ((c + d) % 4) + 128 * h, 128)
        push(i, terms.at[q(2, 0)], r1.at[i, 0, pl.ds(0, 128)], opp1.at[i, 0], to(1))
        push(i, terms.at[q(2, 1)], r1.at[i, 1, pl.ds(0, 128)], opp1.at[i, 1], to(3))
        push(i, terms.at[q(1, 1)], r1.at[i, 0, pl.ds(256, 128)], rest1.at[i, 0], to(1))
        push(i, terms.at[q(3, 0)], r1.at[i, 1, pl.ds(128, 128)], rest1.at[i, 1], to(3))

    def e1(i):
        (c, to), _, _ = place(i)
        base, s = i * D, i % SLOTS
        for side, (d, h) in enumerate(((1, 0), (3, 1))):
            arrived(r1.at[i, side, pl.ds(0, 128)], opp1.at[i, side])
            own = terms[rows(base + 256 * ((c + d) % 4) + 128 * h, 128), :].astype(F32)
            c1[s, side] = (own + r1[i, side, pl.ds(0, 128)].astype(F32)).astype(BF)
            push(i, c1.at[s, side], r1.at[i, side, pl.ds(128 + 128 * h, 128)], rest1.at[i, side], to(d))

    def e2(i):
        (c, _), (d2, to), _ = place(i)
        base, s, f = i * D, i % SLOTS, i % FSLOTS
        for side in range(2):
            arrived(r1.at[i, side, pl.ds(128, 256)], rest1.at[i, side])
        f1[f] = (terms[rows(base + 256 * c, 256), :].astype(F32)
                 + r1[i, 0, pl.ds(128, 256)].astype(F32) + r1[i, 1, pl.ds(128, 256)].astype(F32))
        s2[s, pl.ds(0, 64)] = f1[f, rows(64 * ((d2 + 2) % 4), 64)].astype(BF)
        s2[s, pl.ds(64, 32)] = f1[f, rows(64 * ((d2 + 1) % 4) + 32, 32)].astype(BF)
        s2[s, pl.ds(96, 32)] = f1[f, rows(64 * ((d2 + 3) % 4), 32)].astype(BF)
        push(i, s2.at[s, pl.ds(0, 32)], r2.at[i, 0, pl.ds(0, 32)], opp2.at[i, 0], to(1))
        push(i, s2.at[s, pl.ds(32, 32)], r2.at[i, 1, pl.ds(0, 32)], opp2.at[i, 1], to(3))
        push(i, s2.at[s, pl.ds(64, 32)], r2.at[i, 0, pl.ds(64, 32)], rest2.at[i, 0], to(1))
        push(i, s2.at[s, pl.ds(96, 32)], r2.at[i, 1, pl.ds(32, 32)], rest2.at[i, 1], to(3))

    def e3(i):
        _, (c, to), _ = place(i)
        s, f = i % SLOTS, i % FSLOTS
        for side, (d, h) in enumerate(((1, 0), (3, 1))):
            arrived(r2.at[i, side, pl.ds(0, 32)], opp2.at[i, side])
            own = f1[f, rows(64 * ((c + d) % 4) + 32 * h, 32)]
            s2[s, pl.ds(128 + 32 * side, 32)] = (own + r2[i, side, pl.ds(0, 32)].astype(F32)).astype(BF)
            push(i, s2.at[s, pl.ds(128 + 32 * side, 32)], r2.at[i, side, pl.ds(32 + 32 * h, 32)],
                 rest2.at[i, side], to(d))

    def e4(i):
        _, (c, _), (d3, to) = place(i)
        s, f = i % SLOTS, i % FSLOTS
        for side in range(2):
            arrived(r2.at[i, side, pl.ds(32, 64)], rest2.at[i, side])
        f2[f] = (f1[f, rows(64 * c, 64)]
                 + r2[i, 0, pl.ds(32, 64)].astype(F32) + r2[i, 1, pl.ds(32, 64)].astype(F32))
        for d in (2, 1, 3):
            s3[s, pl.ds(16 * (d - 1), 16)] = f2[f, rows(16 * ((d3 + d) % 4), 16)].astype(BF)
            push(i, s3.at[s, pl.ds(16 * (d - 1), 16)], r3.at[i, pl.ds(16 * (d - 1), 16)], in3.at[i], to(d))

    def e5(i):
        (p1, _), (p2, _), (p3, to) = place(i)
        f = i % FSLOTS
        arrived(r3.at[i], in3.at[i])
        total = f2[f, rows(16 * p3, 16)]
        for d in range(3):
            total += r3[i, pl.ds(16 * d, 16)].astype(F32)
        mine = rows(i * D + 256 * p1 + 64 * p2 + 16 * p3, 16)
        out[mine, :] = total.astype(BF)
        for d in (2, 1, 3):
            push(i, out.at[mine], out.at[mine], ag3.at[i], to(d))

    def gather(i, base, size, c, to, fwd, rest):
        half = size // 2
        h0, h1 = (out.at[rows(base + size * c + half * h, half)] for h in range(2))
        push(i, h0, h0, fwd.at[i, 0], to(1))
        push(i, h1, h1, fwd.at[i, 1], to(3))
        push(i, h1, h1, rest.at[i, 0], to(1))
        push(i, h0, h0, rest.at[i, 1], to(3))

    def onward(i, base, size, c, to, fwd, rest):
        half = size // 2
        for side, (d, h) in enumerate(((1, 0), (3, 1))):
            ref = out.at[rows(base + size * ((c - d) % 4) + half * h, half)]
            arrived(ref, fwd.at[i, side])
            push(i, ref, ref, rest.at[i, side], to(d))

    def e6(i):
        (p1, _), (p2, to), _ = place(i)
        arrived(out.at[pl.ds(0, 48)], ag3.at[i])
        gather(i, i * D + 256 * p1, 64, p2, to, fwd2, ag2)

    def e7(i):
        (p1, _), (p2, to), _ = place(i)
        onward(i, i * D + 256 * p1, 64, p2, to, fwd2, ag2)

    def e8(i):
        (p1, to), _, _ = place(i)
        for side in range(2):
            arrived(out.at[pl.ds(0, 64)], ag2.at[i, side])
        gather(i, i * D, 256, p1, to, fwd1, ag1)

    def e9(i):
        (p1, to), _, _ = place(i)
        onward(i, i * D, 256, p1, to, fwd1, ag1)

    def e10(i):
        for side in range(2):
            arrived(out.at[pl.ds(0, 256)], ag1.at[i, side])
        arrived(terms.at[pl.ds(0, 4 * 512 - 32)], send.at[i % SLOTS])

    events = (e0, e1, e2, e3, e4, e5, e6, e7, e8, e9, e10)

    g_start(0)
    for j in range(TOKENS // KB):
        a_copy(0, j).start()
    barrier = pltpu.get_barrier_semaphore()
    for k in range(3):
        _, to = axis(k)
        for d in range(1, 4):
            pl.semaphore_signal(barrier, inc=1, device_id={"dp": to(d)}, device_id_type=MESH)
    pl.semaphore_wait(barrier, 9)

    def slot(t, carry):
        g_start(t + 1)

        @pl.when(t < ITEMS)
        def _():
            g_wait(t)

        @pl.when(t == 0)
        def _():
            blocked(0, slice(None), 0, lambda j: a_copy(0, j).wait(), lambda j: None)

        @pl.when(t == MIXED)
        def _():
            blocked(MIXED % 2, slice(0, 128), MIXED * D, lambda j: None, lambda j: a_copy(1, j).start())
            blocked(MIXED % 2, slice(128, 256), MIXED * D, lambda j: a_copy(1, j).wait(), lambda j: None)

        @pl.when((t > 0) & (t < ITEMS) & (t != MIXED))
        def _():
            terms[rows(t * D, D), :] = dot(a_buf[...], g_buf[t % 2]).astype(BF)

        for lag, event in zip(LAGS, events):
            i = t - lag

            @pl.when((i >= 0) & (i < ITEMS))
            def _():
                event(i)

        return carry

    lax.fori_loop(0, ITEMS + LAGS[10], slot, 0)


def spread(src, dst, sem):
    copies = []
    for i in range(ITEMS):
        if i == MIXED:
            for n in range(2):
                copies.append((src.at[pl.ds(i * D, D), pl.ds(128 * n, 128)], dst.at[n, :, pl.ds(PER * COLS, 128)]))
        else:
            n = i // (MIXED + 1)
            b = i - n * (MIXED + 1)
            copies.append((src.at[pl.ds(i * D, D), :], dst.at[n, :, pl.ds(b * COLS, COLS)]))
    copies = [pltpu.make_async_copy(s, d, sem.at[j]) for j, (s, d) in enumerate(copies)]
    for c in copies:
        c.start()
    for c in copies:
        c.wait()


def solution(mesh):
    def step(a, g):
        dma = pltpu.SemaphoreType.DMA
        sums = pl.pallas_call(
            kernel,
            out_shape=pltpu.VMEM((ITEMS * D, COLS), BF),
            in_specs=[pl.BlockSpec(memory_space=pltpu.HBM)] * 2,
            out_specs=pl.BlockSpec(memory_space=pltpu.VMEM),
            scratch_shapes=[
                pltpu.VMEM((TOKENS, D), BF),
                pltpu.VMEM((2, TOKENS, COLS), BF),
                pltpu.VMEM((D, COLS), F32),
                pltpu.VMEM((ITEMS * D, COLS), BF),
                pltpu.VMEM((ITEMS, 2, 384, COLS), BF),
                pltpu.VMEM((SLOTS, 2, 128, COLS), BF),
                pltpu.VMEM((FSLOTS, 256, COLS), F32),
                pltpu.VMEM((SLOTS, 192, COLS), BF),
                pltpu.VMEM((ITEMS, 2, 96, COLS), BF),
                pltpu.VMEM((FSLOTS, 64, COLS), F32),
                pltpu.VMEM((SLOTS, 48, COLS), BF),
                pltpu.VMEM((ITEMS, 48, COLS), BF),
                dma((TOKENS // KB,)),
                dma((2,)),
                dma((SLOTS,)),
                dma((ITEMS, 2)),
                dma((ITEMS, 2)),
                dma((ITEMS, 2)),
                dma((ITEMS, 2)),
                dma((ITEMS,)),
                dma((ITEMS,)),
                dma((ITEMS, 2)),
                dma((ITEMS, 2)),
                dma((ITEMS, 2)),
                dma((ITEMS, 2)),
            ],
            compiler_params=pltpu.CompilerParams(
                collective_id=0, has_side_effects=True, vmem_limit_bytes=50 * 2**20),
        )(a, g)
        return pl.pallas_call(
            spread,
            out_shape=jax.ShapeDtypeStruct((2, D, FF), BF),
            in_specs=[pl.BlockSpec(memory_space=pltpu.VMEM)],
            out_specs=pl.BlockSpec(memory_space=pltpu.HBM),
            scratch_shapes=[dma((ITEMS + 1,))],
            compiler_params=pltpu.CompilerParams(vmem_limit_bytes=2 * 2**20),
        )(sums)

    return jax.shard_map(
        step, mesh=mesh, in_specs=(P(("rep", "dp")), P(("rep", "dp"))), out_specs=P("rep"), check_vma=False)
```

```python
import functools

import jax
import jax.numpy as jnp
from jax import lax
from jax.experimental import pallas as pl
from jax.experimental.pallas import tpu as pltpu
from jax.sharding import PartitionSpec as P

MESH = pl.DeviceIdType.MESH
BF, F32 = jnp.bfloat16, jnp.float32

D, FF, TOKENS = 1024, 3200, 4096
COLS = 256
PER = FF // COLS
ITEMS = 2 * PER + 1
MIXED = PER
KB = 1024
LAGS = (0, 2, 4, 5, 7, 9, 11, 13, 16, 26, 39, 0, 16)
ORDER = (2, 4, 5, 0, 11, 10, 7, 6, 1, 9, 3, 8, 12)
SLOTS = ITEMS
FSLOTS = 8


def kernel(a_hbm, g_hbm, out, a_buf, g_buf, acc, terms, r1, c1, f1, s2, r2, f2, s3, r3,
           a_sem, g_sem, send, opp1, rest1, opp2, rest2, in3, ag3, fwd2, ag2, fwd1, ag1):
    dp, rep = lax.axis_index("dp"), lax.axis_index("rep")
    x, y, z = dp // 16, (dp // 4) % 4, dp % 4

    def axis(n):
        k = (n + rep) % 3
        w0, w1, w2 = (1 - k) * (2 - k) // 2, k * (2 - k), k * (k - 1) // 2
        c, s = x * w0 + y * w1 + z * w2, 16 * w0 + 4 * w1 + w2
        ids = [dp + s * ((c + d) % 4 - c) for d in range(4)]
        return c, lambda d: ids[d]

    axes = [axis(n) for n in range(3)]

    def rows(start, size):
        return pl.ds(pl.multiple_of(start, 16), size)

    def a_copy(n, j):
        return pltpu.make_async_copy(a_hbm.at[0, n, pl.ds(j * KB, KB), :], a_buf.at[pl.ds(j * KB, KB), :], a_sem.at[j])

    def g_copy(n, first, width, slot, at):
        return pltpu.make_async_copy(
            g_hbm.at[0, n, :, pl.ds(first, width)], g_buf.at[slot, :, pl.ds(at, width)], g_sem.at[slot])

    def g_start(t):
        @pl.when((t < MIXED) | ((t > MIXED) & (t < ITEMS)))
        def _():
            n = t // (MIXED + 1)
            b = t - n * (MIXED + 1)
            g_copy(n, pl.multiple_of(b * COLS, COLS), COLS, t % 2, 0).start()

        @pl.when(t == MIXED)
        def _():
            g_copy(0, PER * COLS, 128, MIXED % 2, 0).start()
            g_copy(1, PER * COLS, 128, MIXED % 2, 128).start()

    def g_wait(t):
        g_copy(0, 0, COLS, t % 2, 0).wait()

    def dot(a, g):
        return lax.dot_general(a, g, (((0,), (0,)), ((), ())), preferred_element_type=F32)

    def blocked(slot, cols, row0, before, after):
        for j in range(TOKENS // KB):
            before(j)
            part = dot(a_buf[pl.ds(j * KB, KB), :], g_buf[slot, pl.ds(j * KB, KB), cols])
            if j == 0:
                acc[:, cols] = part
            else:
                acc[:, cols] += part
            after(j)
        terms[pl.ds(row0, D), cols] = acc[:, cols].astype(BF)

    def push(i, src, dst, sem, to):
        pltpu.make_async_remote_copy(
            src_ref=src, dst_ref=dst, send_sem=send.at[i], recv_sem=sem,
            device_id={"dp": to}, device_id_type=MESH).start()

    def arrived(ref, sem):
        pltpu.make_async_copy(ref, ref, sem).wait()

    def place(k):
        return axes[k], axes[(k + 1) % 3], axes[(k + 2) % 3]

    def e0(i, k):
        (c, to), _, _ = place(k)
        base = i * D
        q = lambda d, h: rows(base + 256 * ((c + d) % 4) + 128 * h, 128)
        push(i, terms.at[q(2, 0)], r1.at[i, 0, pl.ds(0, 128)], opp1.at[i, 0], to(1))
        push(i, terms.at[q(2, 1)], r1.at[i, 1, pl.ds(0, 128)], opp1.at[i, 1], to(3))

    def e11(i, k):
        (c, to), _, _ = place(k)
        base = i * D
        q = lambda d, h: rows(base + 256 * ((c + d) % 4) + 128 * h, 128)
        push(i, terms.at[q(1, 1)], r1.at[i, 0, pl.ds(256, 128)], rest1.at[i, 0], to(1))
        push(i, terms.at[q(3, 0)], r1.at[i, 1, pl.ds(128, 128)], rest1.at[i, 1], to(3))

    def e1(i, k):
        (c, to), _, _ = place(k)
        base, s = i * D, i
        for side, (d, h) in enumerate(((1, 0), (3, 1))):
            arrived(r1.at[i, side, pl.ds(0, 128)], opp1.at[i, side])
            own = terms[rows(base + 256 * ((c + d) % 4) + 128 * h, 128), :].astype(F32)
            c1[s, side] = (own + r1[i, side, pl.ds(0, 128)].astype(F32)).astype(BF)
            push(i, c1.at[s, side], r1.at[i, side, pl.ds(128 + 128 * h, 128)], rest1.at[i, side], to(d))

    def e2(i, k):
        (c, _), (d2, to), _ = place(k)
        base, s, f = i * D, i, i % FSLOTS
        for side in range(2):
            arrived(r1.at[i, side, pl.ds(128, 256)], rest1.at[i, side])
        f1[f] = (terms[rows(base + 256 * c, 256), :].astype(F32)
                 + r1[i, 0, pl.ds(128, 256)].astype(F32) + r1[i, 1, pl.ds(128, 256)].astype(F32))
        s2[s, pl.ds(0, 64)] = f1[f, rows(64 * ((d2 + 2) % 4), 64)].astype(BF)
        s2[s, pl.ds(64, 32)] = f1[f, rows(64 * ((d2 + 1) % 4) + 32, 32)].astype(BF)
        s2[s, pl.ds(96, 32)] = f1[f, rows(64 * ((d2 + 3) % 4), 32)].astype(BF)
        push(i, s2.at[s, pl.ds(0, 32)], r2.at[i, 0, pl.ds(0, 32)], opp2.at[i, 0], to(1))
        push(i, s2.at[s, pl.ds(32, 32)], r2.at[i, 1, pl.ds(0, 32)], opp2.at[i, 1], to(3))
        push(i, s2.at[s, pl.ds(64, 32)], r2.at[i, 0, pl.ds(64, 32)], rest2.at[i, 0], to(1))
        push(i, s2.at[s, pl.ds(96, 32)], r2.at[i, 1, pl.ds(32, 32)], rest2.at[i, 1], to(3))

    def e3(i, k):
        _, (c, to), _ = place(k)
        s, f = i, i % FSLOTS
        for side, (d, h) in enumerate(((1, 0), (3, 1))):
            arrived(r2.at[i, side, pl.ds(0, 32)], opp2.at[i, side])
            own = f1[f, rows(64 * ((c + d) % 4) + 32 * h, 32)]
            s2[s, pl.ds(128 + 32 * side, 32)] = (own + r2[i, side, pl.ds(0, 32)].astype(F32)).astype(BF)
            push(i, s2.at[s, pl.ds(128 + 32 * side, 32)], r2.at[i, side, pl.ds(32 + 32 * h, 32)],
                 rest2.at[i, side], to(d))

    def e4(i, k):
        _, (c, _), (d3, to) = place(k)
        s, f = i, i % FSLOTS
        for side in range(2):
            arrived(r2.at[i, side, pl.ds(32, 64)], rest2.at[i, side])
        f2[f] = (f1[f, rows(64 * c, 64)]
                 + r2[i, 0, pl.ds(32, 64)].astype(F32) + r2[i, 1, pl.ds(32, 64)].astype(F32))
        for d in (2, 1, 3):
            s3[s, pl.ds(16 * (d - 1), 16)] = f2[f, rows(16 * ((d3 + d) % 4), 16)].astype(BF)
            push(i, s3.at[s, pl.ds(16 * (d - 1), 16)], r3.at[i, pl.ds(16 * (d - 1), 16)], in3.at[i], to(d))

    def e5(i, k):
        (p1, _), (p2, _), (p3, to) = place(k)
        f = i % FSLOTS
        arrived(r3.at[i], in3.at[i])
        total = f2[f, rows(16 * p3, 16)]
        for d in range(3):
            total += r3[i, pl.ds(16 * d, 16)].astype(F32)
        mine = rows(i * D + 256 * p1 + 64 * p2 + 16 * p3, 16)
        out[mine, :] = total.astype(BF)
        for d in (2, 1, 3):
            push(i, out.at[mine], out.at[mine], ag3.at[i], to(d))

    def halves(base, size, c):
        half = size // 2
        return [out.at[rows(base + size * c + half * h, half)] for h in range(2)]

    def gather(i, base, size, c, to, fwd):
        h0, h1 = halves(base, size, c)
        push(i, h0, h0, fwd.at[i, 0], to(1))
        push(i, h1, h1, fwd.at[i, 1], to(3))

    def others(i, base, size, c, to, rest):
        h0, h1 = halves(base, size, c)
        push(i, h1, h1, rest.at[i, 0], to(1))
        push(i, h0, h0, rest.at[i, 1], to(3))

    def onward(i, base, size, c, to, fwd, rest):
        half = size // 2
        for side, (d, h) in enumerate(((1, 0), (3, 1))):
            ref = out.at[rows(base + size * ((c - d) % 4) + half * h, half)]
            arrived(ref, fwd.at[i, side])
            push(i, ref, ref, rest.at[i, side], to(d))

    def e6(i, k):
        (p1, _), (p2, to), _ = place(k)
        arrived(out.at[pl.ds(0, 48)], ag3.at[i])
        gather(i, i * D + 256 * p1, 64, p2, to, fwd2)
        others(i, i * D + 256 * p1, 64, p2, to, ag2)

    def e7(i, k):
        (p1, _), (p2, to), _ = place(k)
        onward(i, i * D + 256 * p1, 64, p2, to, fwd2, ag2)

    def e8(i, k):
        (p1, to), _, _ = place(k)
        for side in range(2):
            arrived(out.at[pl.ds(0, 64)], ag2.at[i, side])
        gather(i, i * D, 256, p1, to, fwd1)

    def e12(i, k):
        (p1, to), _, _ = place(k)
        others(i, i * D, 256, p1, to, ag1)

    def e9(i, k):
        (p1, to), _, _ = place(k)
        onward(i, i * D, 256, p1, to, fwd1, ag1)

    def e10(i, k):
        for side in range(2):
            arrived(out.at[pl.ds(0, 256)], ag1.at[i, side])
        arrived(terms.at[pl.ds(0, 4 * 512 - 32)], send.at[i])

    events = (e0, e1, e2, e3, e4, e5, e6, e7, e8, e9, e10, e11, e12)

    g_start(0)
    for j in range(TOKENS // KB):
        a_copy(0, j).start()
    g_start(1)
    barrier = pltpu.get_barrier_semaphore()
    for k in range(3):
        _, to = axes[k]
        for d in range(1, 4):
            pl.semaphore_signal(barrier, inc=1, device_id={"dp": to(d)}, device_id_type=MESH)
    g_wait(0)
    blocked(0, slice(None), 0, lambda j: a_copy(0, j).wait(), lambda j: None)
    pl.semaphore_wait(barrier, 9)

    def multiply(t, first):
        @pl.when(t > 0)
        def _():
            g_start(t + 1)

        @pl.when((t > 0) & (t < ITEMS))
        def _():
            g_wait(t)

        if first:
            @pl.when(t == MIXED)
            def _():
                blocked(MIXED % 2, slice(0, 128), MIXED * D, lambda j: None, lambda j: a_copy(1, j).start())
                blocked(MIXED % 2, slice(128, 256), MIXED * D, lambda j: a_copy(1, j).wait(), lambda j: None)

        @pl.when(((t > 0) & (t < ITEMS) & (t != MIXED)) if first else t < ITEMS)
        def _():
            terms[rows(t * D, D), :] = dot(a_buf[...], g_buf[t % 2]).astype(BF)

    def around(r, carry):
        for c in range(3):
            multiply(3 * r + c, c == 0)
            for e in ORDER:
                i = 3 * r + c - LAGS[e]

                @pl.when((i >= 0) & (i < ITEMS))
                def _():
                    events[e](i, (c - LAGS[e]) % 3)

        return carry

    lax.fori_loop(0, (ITEMS + LAGS[10] + 2) // 3, around, 0)


def spread(src, dst, sem):
    copies = []
    for i in range(ITEMS):
        if i == MIXED:
            for n in range(2):
                copies.append((src.at[pl.ds(i * D, D), pl.ds(128 * n, 128)], dst.at[n, :, pl.ds(PER * COLS, 128)]))
        else:
            n = i // (MIXED + 1)
            b = i - n * (MIXED + 1)
            copies.append((src.at[pl.ds(i * D, D), :], dst.at[n, :, pl.ds(b * COLS, COLS)]))
    copies = [pltpu.make_async_copy(s, d, sem.at[j]) for j, (s, d) in enumerate(copies)]
    for c in copies:
        c.start()
    for c in copies:
        c.wait()


def solution(mesh):
    def step(a, g):
        dma = pltpu.SemaphoreType.DMA
        sums = pl.pallas_call(
            kernel,
            out_shape=pltpu.VMEM((ITEMS * D, COLS), BF),
            in_specs=[pl.BlockSpec(memory_space=pltpu.HBM)] * 2,
            out_specs=pl.BlockSpec(memory_space=pltpu.VMEM),
            scratch_shapes=[
                pltpu.VMEM((TOKENS, D), BF),
                pltpu.VMEM((2, TOKENS, COLS), BF),
                pltpu.VMEM((D, COLS), F32),
                pltpu.VMEM((ITEMS * D, COLS), BF),
                pltpu.VMEM((ITEMS, 2, 384, COLS), BF),
                pltpu.VMEM((SLOTS, 2, 128, COLS), BF),
                pltpu.VMEM((FSLOTS, 256, COLS), F32),
                pltpu.VMEM((SLOTS, 192, COLS), BF),
                pltpu.VMEM((ITEMS, 2, 96, COLS), BF),
                pltpu.VMEM((FSLOTS, 64, COLS), F32),
                pltpu.VMEM((SLOTS, 48, COLS), BF),
                pltpu.VMEM((ITEMS, 48, COLS), BF),
                dma((TOKENS // KB,)),
                dma((2,)),
                dma((SLOTS,)),
                dma((ITEMS, 2)),
                dma((ITEMS, 2)),
                dma((ITEMS, 2)),
                dma((ITEMS, 2)),
                dma((ITEMS,)),
                dma((ITEMS,)),
                dma((ITEMS, 2)),
                dma((ITEMS, 2)),
                dma((ITEMS, 2)),
                dma((ITEMS, 2)),
            ],
            compiler_params=pltpu.CompilerParams(
                collective_id=0, has_side_effects=True, vmem_limit_bytes=51 * 2**20),
        )(a, g)
        return pl.pallas_call(
            spread,
            out_shape=jax.ShapeDtypeStruct((2, D, FF), BF),
            in_specs=[pl.BlockSpec(memory_space=pltpu.VMEM)],
            out_specs=pl.BlockSpec(memory_space=pltpu.HBM),
            scratch_shapes=[dma((ITEMS + 1,))],
            compiler_params=pltpu.CompilerParams(vmem_limit_bytes=2 * 2**20),
        )(sums)

    return jax.shard_map(
        step, mesh=mesh, in_specs=(P(("rep", "dp")), P(("rep", "dp"))), out_specs=P("rep"), check_vma=False)
```

```python
import functools

import jax
import jax.numpy as jnp
from jax import lax
from jax.experimental import pallas as pl
from jax.experimental.pallas import tpu as pltpu
from jax.sharding import PartitionSpec as P

MESH = pl.DeviceIdType.MESH
BF, F32 = jnp.bfloat16, jnp.float32

D, FF, TOKENS = 1024, 3200, 4096
COLS = 256
PER = FF // COLS
ITEMS = 2 * PER + 1
MIXED = PER
KB = 2048
LAGS = (0, 2, 4, 0, 7, 9, 11, 0, 14, 27, 41, 0, 14)
ORDER = (2, 4, 5, 0, 11, 10, 6, 1, 9, 8, 12)
SLOTS = ITEMS
FSLOTS = 8


def kernel(a_hbm, g_hbm, out, a_buf, g_buf, acc, terms, r1, c1, f1, s2, r2, f2, s3, r3,
           a_sem, g_sem, send, opp1, rest1, in2, in3, ag3, ag2, fwd1, ag1):
    dp, rep = lax.axis_index("dp"), lax.axis_index("rep")
    x, y, z = dp // 16, (dp // 4) % 4, dp % 4

    def axis(n):
        k = (n + rep) % 3
        w0, w1, w2 = (1 - k) * (2 - k) // 2, k * (2 - k), k * (k - 1) // 2
        c, s = x * w0 + y * w1 + z * w2, 16 * w0 + 4 * w1 + w2
        ids = [dp + s * ((c + d) % 4 - c) for d in range(4)]
        return c, lambda d: ids[d]

    axes = [axis(n) for n in range(3)]

    def rows(start, size):
        return pl.ds(pl.multiple_of(start, 16), size)

    def a_copy(n, j):
        return pltpu.make_async_copy(a_hbm.at[0, n, pl.ds(j * KB, KB), :], a_buf.at[pl.ds(j * KB, KB), :], a_sem.at[j])

    def g_copy(n, first, width, slot, at):
        return pltpu.make_async_copy(
            g_hbm.at[0, n, :, pl.ds(first, width)], g_buf.at[slot, :, pl.ds(at, width)], g_sem.at[slot])

    def g_start(t):
        @pl.when((t < MIXED) | ((t > MIXED) & (t < ITEMS)))
        def _():
            n = t // (MIXED + 1)
            b = t - n * (MIXED + 1)
            g_copy(n, pl.multiple_of(b * COLS, COLS), COLS, t % 2, 0).start()

        @pl.when(t == MIXED)
        def _():
            g_copy(0, PER * COLS, 128, MIXED % 2, 0).start()
            g_copy(1, PER * COLS, 128, MIXED % 2, 128).start()

    def g_wait(t):
        g_copy(0, 0, COLS, t % 2, 0).wait()

    def dot(a, g):
        return lax.dot_general(a, g, (((0,), (0,)), ((), ())), preferred_element_type=F32)

    def blocked(slot, cols, row0, before, after):
        for j in range(TOKENS // KB):
            before(j)
            part = dot(a_buf[pl.ds(j * KB, KB), :], g_buf[slot, pl.ds(j * KB, KB), cols])
            if j == 0:
                acc[:, cols] = part
            else:
                acc[:, cols] += part
            after(j)
        terms[pl.ds(row0, D), cols] = acc[:, cols].astype(BF)

    def push(i, src, dst, sem, to):
        pltpu.make_async_remote_copy(
            src_ref=src, dst_ref=dst, send_sem=send.at[i], recv_sem=sem,
            device_id={"dp": to}, device_id_type=MESH).start()

    def arrived(ref, sem):
        pltpu.make_async_copy(ref, ref, sem).wait()

    def place(k):
        return axes[k], axes[(k + 1) % 3], axes[(k + 2) % 3]

    def e0(i, k):
        (c, to), _, _ = place(k)
        base = i * D
        q = lambda d, h: rows(base + 256 * ((c + d) % 4) + 128 * h, 128)
        push(i, terms.at[q(2, 0)], r1.at[i, 0, pl.ds(0, 128)], opp1.at[i, 0], to(1))
        push(i, terms.at[q(2, 1)], r1.at[i, 1, pl.ds(0, 128)], opp1.at[i, 1], to(3))

    def e11(i, k):
        (c, to), _, _ = place(k)
        base = i * D
        q = lambda d, h: rows(base + 256 * ((c + d) % 4) + 128 * h, 128)
        push(i, terms.at[q(1, 1)], r1.at[i, 0, pl.ds(256, 128)], rest1.at[i, 0], to(1))
        push(i, terms.at[q(3, 0)], r1.at[i, 1, pl.ds(128, 128)], rest1.at[i, 1], to(3))

    def e1(i, k):
        (c, to), _, _ = place(k)
        base, s = i * D, i
        for side, (d, h) in enumerate(((1, 0), (3, 1))):
            arrived(r1.at[i, side, pl.ds(0, 128)], opp1.at[i, side])
            own = terms[rows(base + 256 * ((c + d) % 4) + 128 * h, 128), :].astype(F32)
            c1[s, side] = (own + r1[i, side, pl.ds(0, 128)].astype(F32)).astype(BF)
            push(i, c1.at[s, side], r1.at[i, side, pl.ds(128 + 128 * h, 128)], rest1.at[i, side], to(d))

    def e2(i, k):
        (c, _), (d2, to), _ = place(k)
        base, s, f = i * D, i, i % FSLOTS
        for side in range(2):
            arrived(r1.at[i, side, pl.ds(128, 256)], rest1.at[i, side])
        f1[f] = (terms[rows(base + 256 * c, 256), :].astype(F32)
                 + r1[i, 0, pl.ds(128, 256)].astype(F32) + r1[i, 1, pl.ds(128, 256)].astype(F32))
        for d in (2, 1, 3):
            piece = pl.ds(64 * (d - 1), 64)
            s2[s, piece] = f1[f, rows(64 * ((d2 + d) % 4), 64)].astype(BF)
            push(i, s2.at[s, piece], r2.at[i, piece], in2.at[i], to(d))

    def e4(i, k):
        _, (c, _), (d3, to) = place(k)
        s, f = i, i % FSLOTS
        arrived(r2.at[i], in2.at[i])
        total = f1[f, rows(64 * c, 64)]
        for d in range(3):
            total += r2[i, pl.ds(64 * d, 64)].astype(F32)
        f2[f] = total
        for d in (2, 1, 3):
            s3[s, pl.ds(16 * (d - 1), 16)] = f2[f, rows(16 * ((d3 + d) % 4), 16)].astype(BF)
            push(i, s3.at[s, pl.ds(16 * (d - 1), 16)], r3.at[i, pl.ds(16 * (d - 1), 16)], in3.at[i], to(d))

    def e5(i, k):
        (p1, _), (p2, _), (p3, to) = place(k)
        f = i % FSLOTS
        arrived(r3.at[i], in3.at[i])
        total = f2[f, rows(16 * p3, 16)]
        for d in range(3):
            total += r3[i, pl.ds(16 * d, 16)].astype(F32)
        mine = rows(i * D + 256 * p1 + 64 * p2 + 16 * p3, 16)
        out[mine, :] = total.astype(BF)
        for d in (2, 1, 3):
            push(i, out.at[mine], out.at[mine], ag3.at[i], to(d))

    def halves(base, size, c):
        half = size // 2
        return [out.at[rows(base + size * c + half * h, half)] for h in range(2)]

    def gather(i, base, size, c, to, fwd):
        h0, h1 = halves(base, size, c)
        push(i, h0, h0, fwd.at[i, 0], to(1))
        push(i, h1, h1, fwd.at[i, 1], to(3))

    def others(i, base, size, c, to, rest):
        h0, h1 = halves(base, size, c)
        push(i, h1, h1, rest.at[i, 0], to(1))
        push(i, h0, h0, rest.at[i, 1], to(3))

    def onward(i, base, size, c, to, fwd, rest):
        half = size // 2
        for side, (d, h) in enumerate(((1, 0), (3, 1))):
            ref = out.at[rows(base + size * ((c - d) % 4) + half * h, half)]
            arrived(ref, fwd.at[i, side])
            push(i, ref, ref, rest.at[i, side], to(d))

    def e6(i, k):
        (p1, _), (p2, to), _ = place(k)
        arrived(out.at[pl.ds(0, 48)], ag3.at[i])
        mine = out.at[rows(i * D + 256 * p1 + 64 * p2, 64)]
        for d in (2, 1, 3):
            push(i, mine, mine, ag2.at[i], to(d))

    def e8(i, k):
        (p1, to), _, _ = place(k)
        arrived(out.at[pl.ds(0, 192)], ag2.at[i])
        gather(i, i * D, 256, p1, to, fwd1)

    def e12(i, k):
        (p1, to), _, _ = place(k)
        others(i, i * D, 256, p1, to, ag1)

    def e9(i, k):
        (p1, to), _, _ = place(k)
        onward(i, i * D, 256, p1, to, fwd1, ag1)

    def e10(i, k):
        for side in range(2):
            arrived(out.at[pl.ds(0, 256)], ag1.at[i, side])
        arrived(terms.at[pl.ds(0, 4 * 512 - 32)], send.at[i])

    events = (e0, e1, e2, None, e4, e5, e6, None, e8, e9, e10, e11, e12)

    g_start(0)
    for j in range(TOKENS // KB):
        a_copy(0, j).start()
    g_start(1)
    barrier = pltpu.get_barrier_semaphore()
    for k in range(3):
        _, to = axes[k]
        for d in range(1, 4):
            pl.semaphore_signal(barrier, inc=1, device_id={"dp": to(d)}, device_id_type=MESH)
    g_wait(0)
    blocked(0, slice(None), 0, lambda j: a_copy(0, j).wait(), lambda j: None)
    pl.semaphore_wait(barrier, 9)

    def multiply(t, first):
        @pl.when(t > 0)
        def _():
            g_start(t + 1)

        @pl.when((t > 0) & (t < ITEMS))
        def _():
            g_wait(t)

        if first:
            @pl.when(t == MIXED)
            def _():
                blocked(MIXED % 2, slice(0, 128), MIXED * D, lambda j: None, lambda j: a_copy(1, j).start())
                blocked(MIXED % 2, slice(128, 256), MIXED * D, lambda j: a_copy(1, j).wait(), lambda j: None)

        @pl.when(((t > 0) & (t < ITEMS) & (t != MIXED)) if first else t < ITEMS)
        def _():
            terms[rows(t * D, D), :] = dot(a_buf[...], g_buf[t % 2]).astype(BF)

    def around(r, carry):
        for c in range(3):
            multiply(3 * r + c, c == 0)
            for e in ORDER:
                i = 3 * r + c - LAGS[e]

                @pl.when((i >= 0) & (i < ITEMS))
                def _():
                    events[e](i, (c - LAGS[e]) % 3)

        return carry

    lax.fori_loop(0, (ITEMS + LAGS[10] + 2) // 3, around, 0)


def spread(src, dst, sem):
    copies = []
    for i in range(ITEMS):
        if i == MIXED:
            for n in range(2):
                copies.append((src.at[pl.ds(i * D, D), pl.ds(128 * n, 128)], dst.at[n, :, pl.ds(PER * COLS, 128)]))
        else:
            n = i // (MIXED + 1)
            b = i - n * (MIXED + 1)
            copies.append((src.at[pl.ds(i * D, D), :], dst.at[n, :, pl.ds(b * COLS, COLS)]))
    copies = [pltpu.make_async_copy(s, d, sem.at[j]) for j, (s, d) in enumerate(copies)]
    for c in copies:
        c.start()
    for c in copies:
        c.wait()


def solution(mesh):
    def step(a, g):
        dma = pltpu.SemaphoreType.DMA
        sums = pl.pallas_call(
            kernel,
            out_shape=pltpu.VMEM((ITEMS * D, COLS), BF),
            in_specs=[pl.BlockSpec(memory_space=pltpu.HBM)] * 2,
            out_specs=pl.BlockSpec(memory_space=pltpu.VMEM),
            scratch_shapes=[
                pltpu.VMEM((TOKENS, D), BF),
                pltpu.VMEM((2, TOKENS, COLS), BF),
                pltpu.VMEM((D, COLS), F32),
                pltpu.VMEM((ITEMS * D, COLS), BF),
                pltpu.VMEM((ITEMS, 2, 384, COLS), BF),
                pltpu.VMEM((SLOTS, 2, 128, COLS), BF),
                pltpu.VMEM((FSLOTS, 256, COLS), F32),
                pltpu.VMEM((SLOTS, 192, COLS), BF),
                pltpu.VMEM((ITEMS, 192, COLS), BF),
                pltpu.VMEM((FSLOTS, 64, COLS), F32),
                pltpu.VMEM((SLOTS, 48, COLS), BF),
                pltpu.VMEM((ITEMS, 48, COLS), BF),
                dma((TOKENS // KB,)),
                dma((2,)),
                dma((SLOTS,)),
                dma((ITEMS, 2)),
                dma((ITEMS, 2)),
                dma((ITEMS,)),
                dma((ITEMS,)),
                dma((ITEMS,)),
                dma((ITEMS,)),
                dma((ITEMS, 2)),
                dma((ITEMS, 2)),
            ],
            compiler_params=pltpu.CompilerParams(
                collective_id=0, has_side_effects=True, vmem_limit_bytes=51 * 2**20),
        )(a, g)
        return pl.pallas_call(
            spread,
            out_shape=jax.ShapeDtypeStruct((2, D, FF), BF),
            in_specs=[pl.BlockSpec(memory_space=pltpu.VMEM)],
            out_specs=pl.BlockSpec(memory_space=pltpu.HBM),
            scratch_shapes=[dma((ITEMS + 1,))],
            compiler_params=pltpu.CompilerParams(vmem_limit_bytes=2 * 2**20),
        )(sums)

    return jax.shard_map(
        step, mesh=mesh, in_specs=(P(("rep", "dp")), P(("rep", "dp"))), out_specs=P("rep"), check_vma=False)
```
